32 devices in a mesh: pa: 4 (over y, x), pb: 8 (over z, core).
Axes of the slice: x: 2, y: 2, z: 4, core: 2. Of those that a mesh axis runs over, the one named last changes fastest.
Arguments:
- right_side: float32 [32, 64, 128], P(None, 'pa', 'pb'), may hold values from -6 to 6
- coef_x: float32 [32, 64, 128], P(None, 'pa', 'pb'), may hold values from 0.1 to 4
- coef_y: float32 [32, 64, 128], P(None, 'pa', 'pb'), may hold values from 0.1 to 4
- coef_z: float32 [32, 64, 128], P(None, 'pa', 'pb'), may hold values from 0.1 to 4
Outputs:
- solution_field: float32 [32, 64, 128], P(None, 'pa', 'pb')
- residual: float32 [32, 64, 128], P(None, 'pa', 'pb')
The draws below stay inside these ranges and needn't reach their ends.
All inputs are finite; a program needn't handle non-finite values.
Results may differ from the reference program's by a relative error of at most 0.0003.
Values sent between devices are 32-bit elements.
A program may use at most 64 MiB of HBM per device.

```python
import math
import jax
import jax.numpy as jnp

ITERS = 4
NX = 32
NY = 64
NZ = 128


def block_scale(own_key, shape, shards, least, top_value):
    def one(axis_at, shards_of):
        steps = jax.random.uniform(jax.random.fold_in(jax.random.fold_in(own_key, 6), axis_at), (shards_of,), jnp.float32, least / len(shards), top_value / len(shards))
        return jnp.repeat(jnp.exp(steps), shape[axis_at] // shards_of).reshape((-1,) + (1,) * (len(shape) - axis_at - 1))

    gain = one(*shards[0])
    for cut in shards[1:]:
        gain = gain * one(*cut)
    return gain


def scatter_about(stream_key, extent, spread, bound, shards=(), held_as=jnp.bfloat16):
    loudness = block_scale(stream_key, extent, shards, -0.22, 0.18) if shards else 1.0
    entries = jax.random.normal(stream_key, extent, jnp.float32) * spread * loudness
    return jnp.minimum(jnp.maximum(entries, -bound), bound).astype(held_as)


def setup_inputs(seed: int = 0) -> dict:
    arg_keys = jax.random.split(jax.random.key(seed), 5)
    right_side = scatter_about(arg_keys[0], (NX, NY, NZ), 1.0, 6.0, ((1, 4), (2, 8)), jnp.float32)
    coef_x = jnp.clip(jnp.exp(math.log(4.0) - 3.6888794 * jax.random.uniform(arg_keys[1], (NX, NY, NZ), jnp.float32) ** block_scale(arg_keys[1], (NX, NY, NZ), ((1, 4), (2, 8)), -0.2, 0.2)), 0.1, 4.0)
    coef_y = jnp.clip(jnp.exp(math.log(4.0) - 3.6888794 * jax.random.uniform(arg_keys[2], (NX, NY, NZ), jnp.float32) ** block_scale(arg_keys[2], (NX, NY, NZ), ((1, 4), (2, 8)), -0.2, 0.2)), 0.1, 4.0)
    coef_z = jnp.clip(jnp.exp(math.log(4.0) - 3.6888794 * jax.random.uniform(arg_keys[3], (NX, NY, NZ), jnp.float32) ** block_scale(arg_keys[3], (NX, NY, NZ), ((1, 4), (2, 8)), -0.2, 0.2)), 0.1, 4.0)
    return {"right_side": right_side, "coef_x": coef_x, "coef_y": coef_y, "coef_z": coef_z}


mass_shift = 0.5
base_coef = 1.0


def wave_term(points):
    positions = jnp.arange(points).astype(jnp.float32)
    return 2.0 - 2.0 * jnp.cos(2.0 * jnp.pi * positions / points)


def precondition(grid_field):
    symbol = mass_shift + base_coef * (wave_term(NX)[:, None, None] + wave_term(NY)[None, :, None] + wave_term(NZ)[None, None, :])
    spectrum = jnp.fft.fftn(grid_field)
    return jnp.real(jnp.fft.ifftn(spectrum / symbol)).astype(jnp.float32)


def operate(grid_field, coef_x, coef_y, coef_z):
    result = mass_shift * grid_field
    for axis_number, weights in ((0, coef_x), (1, coef_y), (2, coef_z)):
        above_cells = jnp.roll(grid_field, -1, axis_number)
        below_cells = jnp.roll(grid_field, 1, axis_number)
        weights_low = jnp.roll(weights, 1, axis_number)
        result = result + weights * (grid_field - above_cells) + weights_low * (grid_field - below_cells)
    return result


def reference(right_side, coef_x, coef_y, coef_z):
    solution_field = jnp.zeros_like(right_side)
    residual = right_side
    precond = precondition(residual)
    direction = precond
    fit_now = jnp.sum(residual * precond)
    for iteration in range(ITERS):
        image_field = operate(direction, coef_x, coef_y, coef_z)
        step_size = fit_now / jnp.sum(direction * image_field)
        solution_field = solution_field + step_size * direction
        residual = residual - step_size * image_field
        if iteration + 1 < ITERS:
            precond = precondition(residual)
            fit_next = jnp.sum(residual * precond)
            direction = precond + (fit_next / fit_now) * direction
            fit_now = fit_next
    return solution_field, residual
```

```python
import functools
import math

import jax
import jax.numpy as jnp
import numpy as np
from jax import lax
from jax.experimental import pallas as pl
from jax.experimental.pallas import tpu as pltpu
from jax.sharding import PartitionSpec as P

ITERS = 4
MESH = pl.DeviceIdType.MESH
LANES = 128
mass_shift = 0.5
base_coef = 1.0


def real_basis(points):
    position = np.arange(points)[:, None]
    mode = np.arange(points)[None, :]
    wave = (mode + 1) // 2
    angle = 2.0 * np.pi * ((position * wave) % points) / points
    basis = np.where(mode % 2 == 1, np.cos(angle), np.sin(angle)) * math.sqrt(2.0 / points)
    basis[:, 0] = 1.0 / math.sqrt(points)
    if points % 2 == 0:
        basis[:, -1] = np.cos(np.pi * np.arange(points)) / math.sqrt(points)
    return basis, 2.0 - 2.0 * np.cos(2.0 * np.pi * wave[0] / points)


def halves(matrix):
    high = matrix.astype(np.float32).astype(jnp.bfloat16)
    low = (matrix - high.astype(np.float64)).astype(np.float32).astype(jnp.bfloat16)
    return high, low


def left_table(matrix):
    high, low = halves(matrix)
    return np.concatenate([high, high, low], axis=1)


def right_table(matrix):
    high, low = halves(matrix)
    return np.concatenate([high, high, low], axis=0)


def split(values, axis):
    high = values.astype(jnp.bfloat16)
    low = (values - high.astype(jnp.float32)).astype(jnp.bfloat16)
    return jnp.concatenate([high, low, high], axis=axis)


def left_mul(table, values):
    return jnp.dot(table[...], split(values, 0), preferred_element_type=jnp.float32)


def right_mul(values, table):
    return jnp.dot(split(values, 1), table[...], preferred_element_type=jnp.float32)


def lane_roll(values, by):
    return pltpu.roll(values, by % values.shape[-1], values.ndim - 1)


def row_roll(values, by):
    return pltpu.roll(values, by % values.shape[-2], values.ndim - 2)


def swap_blocks(tile, width):
    row = lax.broadcasted_iota(jnp.int32, tile.shape, 0)
    block = lax.broadcasted_iota(jnp.int32, tile.shape, 1) // width
    for bit in (1, 2, 4):
        row_set = (row // bit) % 2 == 1
        block_set = (block // bit) % 2 == 1
        upper = lane_roll(row_roll(tile, bit), -bit * width)
        lower = lane_roll(row_roll(tile, -bit), bit * width)
        tile = jnp.where(row_set == block_set, tile, jnp.where(row_set, upper, lower))
    return tile


def kernel(
    na, nb, dims,
    right_ref, cx_ref, cy_ref, cz_ref,
    x_fwd, x_inv, y_fwd, y_inv, z_fwd, z_inv, wave_x_ref, wave_yz_ref,
    sol_ref, res_ref,
    send_f, recv_f, send_b, recv_b, send_d, recv_d, edge_y, edge_z,
    send_sem, recv_sem, edge_send, edge_recv, own_sem,
):
    nx, ry, rz = dims
    n = na * nb
    group = LANES // rz
    my_a, my_b = lax.axis_index("pa"), lax.axis_index("pb")
    me = my_a * nb + my_b

    barrier = pltpu.get_barrier_semaphore()

    def greet(step, carry):
        peer = lax.rem(me + step, n)
        pl.semaphore_signal(
            barrier, inc=1, device_id=(peer // nb, lax.rem(peer, nb)), device_id_type=MESH
        )
        return carry

    lax.fori_loop(1, n, greet, 0)
    pl.semaphore_wait(barrier, n - 1)

    def exchange(src, dst, rows, phase, by_peer):
        def own(base):
            return src.at[pl.ds(base, rows), :]

        def send(step, carry):
            peer = lax.rem(me + step, n)
            source = src.at[pl.ds(peer * rows, rows), :] if by_peer else src.at[pl.ds(0, rows), :]
            pltpu.make_async_remote_copy(
                src_ref=source,
                dst_ref=dst.at[pl.ds(me * rows, rows), :],
                send_sem=send_sem.at[phase],
                recv_sem=recv_sem.at[phase],
                device_id=(peer // nb, lax.rem(peer, nb)),
                device_id_type=MESH,
            ).start()
            return carry

        lax.fori_loop(1, n, send, 0, unroll=n <= 32)
        source = src[pl.ds(me * rows, rows), :] if by_peer else src[pl.ds(0, rows), :]
        dst[pl.ds(me * rows, rows), :] = source

    def arrive(dst, rows, phase):
        every = dst.at[pl.ds(0, (n - 1) * rows), :]
        pltpu.make_async_copy(every, every, recv_sem.at[phase]).wait()

    def drain(dst, rows, phase):
        every = dst.at[pl.ds(0, (n - 1) * rows), :]
        pltpu.make_async_copy(every, every, send_sem.at[phase]).wait()

    lane = lax.broadcasted_iota(jnp.int32, (nx, LANES), 1)
    z_at, y_at = lane % rz, lane // rz
    z_first, z_last = z_at == 0, z_at == rz - 1
    y_first, y_last = y_at == 0, y_at == group - 1

    def parts(ref):
        return ref[:, :LANES], ref[:, LANES:]

    def forward(first, second, partial, phase):
        modes = left_mul(x_fwd, jnp.concatenate([first, second], axis=1))
        out = send_f.at[phase]
        out[pl.ds(0, nx, stride=3), :] = modes[:, :LANES]
        out[pl.ds(1, nx, stride=3), :] = modes[:, LANES:]
        out[pl.ds(2, nx, stride=3), :] = jnp.broadcast_to(partial, (nx, LANES))
        exchange(out, recv_f.at[phase], 3, phase, True)

    def plane(phase):
        came = recv_f.at[phase]
        arrive(came, 3, phase)
        rows = []
        for a in range(na):
            for h in range(2):
                tiles = [
                    swap_blocks(came[pl.ds((a * nb + high * 8) * 3 + h, 8, stride=3), :], rz)
                    for high in range(nb // 8)
                ]
                rows.append(tiles[0] if len(tiles) == 1 else jnp.concatenate(tiles, axis=1))
        values = jnp.concatenate(rows, axis=0)
        total = jnp.sum(came[pl.ds(2, n, stride=3), :], keepdims=True)
        return left_mul(y_fwd, right_mul(values, z_fwd)), total

    tile_lane = lax.broadcasted_iota(jnp.int32, (nb, LANES), 1)
    tile_z, tile_y = tile_lane % rz, tile_lane // rz

    def backward(spectrum, partial, phase):
        values = right_mul(left_mul(y_inv, spectrum), z_inv)
        tiles = []
        for a in range(na):
            pair = []
            for h in range(2):
                at = (a * 2 + h) * 8
                cut = [
                    swap_blocks(values[at : at + 8, high * LANES : (high + 1) * LANES], rz)
                    for high in range(nb // 8)
                ]
                pair.append(cut[0] if len(cut) == 1 else jnp.concatenate(cut, axis=0))
            tiles.append(pair)
        out = send_b.at[phase]
        for a in range(na):
            t0, t1 = tiles[a]
            edges_z = jnp.where(
                tile_z == 0,
                row_roll(t0, -1),
                jnp.where(
                    tile_z == 1,
                    lane_roll(row_roll(t1, -1), 1),
                    jnp.where(
                        tile_z == rz - 1,
                        row_roll(t0, 1),
                        lane_roll(row_roll(t1, 1), -1),
                    ),
                ),
            )
            edges_y = jnp.where(
                tile_y == 0,
                tiles[(a + 1) % na][0],
                jnp.where(tile_y == group - 1, tiles[(a - 1) % na][1], partial),
            )
            for j, rows in enumerate((t0, t1, edges_z, edges_y)):
                out[pl.ds(a * nb * 4 + j, nb, stride=4), :] = rows
        exchange(out, recv_b.at[phase], 4, ITERS + phase, True)

    def block(phase):
        came = recv_b.at[phase]
        arrive(came, 4, ITERS + phase)
        pieces = [came[pl.ds(j, nx, stride=4), :] for j in range(4)]
        total = jnp.sum(jnp.where(lane == rz, pieces[3], 0.0), keepdims=True)
        values = left_mul(x_inv, jnp.concatenate(pieces, axis=1))
        return [values[:, j * LANES : (j + 1) * LANES] for j in range(4)], total

    zero_row = jnp.zeros((1, LANES), jnp.float32)
    right = parts(right_ref)
    forward(right[0], right[1], zero_row, 0)

    copies = (
        pltpu.make_async_remote_copy(
            src_ref=cy_ref.at[:, pl.ds(LANES, LANES)],
            dst_ref=edge_y,
            send_sem=edge_send.at[0],
            recv_sem=edge_recv.at[0],
            device_id=(lax.rem(my_a + 1, na), my_b),
            device_id_type=MESH,
        ),
        pltpu.make_async_remote_copy(
            src_ref=cz_ref,
            dst_ref=edge_z,
            send_sem=edge_send.at[1],
            recv_sem=edge_recv.at[1],
            device_id=(my_a, lax.rem(my_b + 1, nb)),
            device_id_type=MESH,
        ),
    )
    for copy in copies:
        copy.start()

    def operate(p, coefs):
        upper, lower = coefs
        edge_of_z, edge_of_y = p[2], p[3]
        above_y = (
            jnp.where(y_last, lane_roll(p[1], -rz), lane_roll(p[0], -rz)),
            jnp.where(y_last, lane_roll(edge_of_y, -rz), lane_roll(p[1], -rz)),
        )
        below_y = (
            jnp.where(y_first, lane_roll(edge_of_y, rz), lane_roll(p[0], rz)),
            jnp.where(y_first, lane_roll(p[0], rz), lane_roll(p[1], rz)),
        )
        result = []
        for h in range(2):
            own = p[h]
            above_z = jnp.where(z_last, lane_roll(edge_of_z, rz - 1 - h), lane_roll(own, -1))
            below_z = jnp.where(z_first, lane_roll(edge_of_z, h + 1 - rz), lane_roll(own, 1))
            total = mass_shift * own
            total = (
                total
                + upper[0][h] * (own - row_roll(own, -1))
                + lower[0][h] * (own - row_roll(own, 1))
            )
            total = total + upper[1][h] * (own - above_y[h]) + lower[1][h] * (own - below_y[h])
            total = total + upper[2][h] * (own - above_z) + lower[2][h] * (own - below_z)
            result.append(total)
        return result

    planes_row = wave_x_ref[pl.ds(me, 1), :1]
    inverse = 1.0 / (mass_shift + base_coef * (planes_row + wave_yz_ref[...]))

    spectrum = direction = coefs = fit_now = step_size = None
    solution_field, residual = None, right
    for iteration in range(ITERS):
        image_hat, inner = plane(iteration)
        if iteration == 0:
            spectrum = image_hat
        else:
            step_size = fit_now / inner
            spectrum = spectrum - step_size * image_hat
        scaled = spectrum * inverse
        backward(scaled, jnp.sum(spectrum * scaled, keepdims=True), iteration)
        if iteration == 0:
            for copy in copies:
                copy.wait()
            cx, cy, cz = parts(cx_ref), parts(cy_ref), parts(cz_ref)
            near_y, near_z = edge_y[...], parts(edge_z)
            lower_x = [row_roll(c, 1) for c in cx]
            lower_y = [
                jnp.where(y_first, lane_roll(near_y, rz), lane_roll(cy[0], rz)),
                jnp.where(y_first, lane_roll(cy[0], rz), lane_roll(cy[1], rz)),
            ]
            lower_z = [
                jnp.where(z_first, lane_roll(near_z[h], 1 - rz), lane_roll(cz[h], 1))
                for h in range(2)
            ]
            coefs = ((cx, cy, cz), (lower_x, lower_y, lower_z))
        else:
            residual = [r - step_size * i for r, i in zip(residual, image)]
            added = [step_size * d for d in direction[:2]]
            solution_field = (
                added if solution_field is None
                else [s + d for s, d in zip(solution_field, added)]
            )
        precond, fit_next = block(iteration)
        if iteration == 0:
            direction = precond
        else:
            ratio = fit_next / fit_now
            direction = [u + ratio * d for u, d in zip(precond, direction)]
        fit_now = fit_next
        image = operate(direction, coefs)
        partial = jnp.sum(direction[0] * image[0] + direction[1] * image[1], axis=0, keepdims=True)
        if iteration + 1 < ITERS:
            forward(image[0], image[1], partial, iteration + 1)

    send_d[...] = jnp.broadcast_to(partial, send_d.shape)
    exchange(send_d, recv_d, 1, 2 * ITERS, False)
    arrive(recv_d, 1, 2 * ITERS)
    step_size = fit_now / jnp.sum(recv_d[...], keepdims=True)
    for h in range(2):
        at = pl.ds(h * LANES, LANES)
        sol_ref[:, at] = solution_field[h] + step_size * direction[h]
        res_ref[:, at] = residual[h] - step_size * image[h]
    for phase in range(ITERS):
        drain(recv_f.at[phase], 3, phase)
        drain(recv_b.at[phase], 4, ITERS + phase)
    drain(recv_d, 1, 2 * ITERS)


def solution(mesh):
    na, nb = mesh.shape["pa"], mesh.shape["pb"]
    n = na * nb

    def on_device(right_side, coef_x, coef_y, coef_z):
        nx, ry, rz = right_side.shape
        cells = ry * rz
        assert nx == n and cells == 2 * LANES and LANES // rz == 8 and nb % 8 == 0
        basis_x, wave_x = real_basis(nx)
        basis_y, wave_y = real_basis(ry * na)
        basis_z, wave_z = real_basis(rz * nb)
        tables = (
            left_table(basis_x.T), left_table(basis_x),
            left_table(basis_y.T), left_table(basis_y),
            right_table(basis_z), right_table(basis_z.T),
            np.broadcast_to(wave_x[:, None], (nx, LANES)).astype(np.float32),
            (wave_y[:, None] + wave_z[None, :]).astype(np.float32),
        )
        flat = [v.reshape(nx, cells) for v in (right_side, coef_x, coef_y, coef_z)]
        shape = jax.ShapeDtypeStruct((nx, cells), jnp.float32)
        vmem = pl.BlockSpec(memory_space=pltpu.VMEM)
        f32 = jnp.float32
        outs = pl.pallas_call(
            functools.partial(kernel, na, nb, (nx, ry, rz)),
            out_shape=(shape, shape),
            in_specs=[vmem] * 12,
            out_specs=(vmem, vmem),
            scratch_shapes=[
                pltpu.VMEM((ITERS, n * 3, LANES), f32),
                pltpu.VMEM((ITERS, n * 3, LANES), f32),
                pltpu.VMEM((ITERS, n * 4, LANES), f32),
                pltpu.VMEM((ITERS, n * 4, LANES), f32),
                pltpu.VMEM((8, LANES), f32),
                pltpu.VMEM((n, LANES), f32),
                pltpu.VMEM((nx, LANES), f32),
                pltpu.VMEM((nx, cells), f32),
                pltpu.SemaphoreType.DMA((2 * ITERS + 1,)),
                pltpu.SemaphoreType.DMA((2 * ITERS + 1,)),
                pltpu.SemaphoreType.DMA((2,)),
                pltpu.SemaphoreType.DMA((2,)),
                pltpu.SemaphoreType.DMA,
            ],
            compiler_params=pltpu.CompilerParams(collective_id=0, has_side_effects=True),
        )(*flat, *[jnp.asarray(t) for t in tables])
        return tuple(o.reshape(nx, ry, rz) for o in outs)

    spec = P(None, "pa", "pb")
    return jax.shard_map(
        on_device, mesh=mesh, in_specs=(spec,) * 4, out_specs=(spec, spec), check_vma=False
    )
```
